32 devices in a mesh: node: 8 (over z, y), rep: 4 (over x, core).
Axes of the slice: x: 2, y: 2, z: 4, core: 2. Of those that a mesh axis runs over, the one named last changes fastest.
Arguments:
- coords: float32 [3, 4096], P(None, 'node'), may hold values from 0 to 2, as said below
- omega: bfloat16 [4096, 512], P('node', 'rep'), may hold values from -6 to 6
- skeleton: int32 [8, 256], P('node', 'rep'), may hold values from 0 to 4095, as said below
Outputs:
- row_sample: bfloat16 [4096, 512], P('node', 'rep')
- col_sample: float32 [4096, 512], P('node', 'rep')
The draws below stay inside these ranges and needn't reach their ends.
Inputs may be any that keep to these rules, and one draw needn't show every extreme that they name: `skeleton`: each node's list holds distinct indices, none inside its own points, at most 73 inside the points of any one other node; in every draw one node's points hold exactly 73 indices of every other node's list. `coords`: the first coordinate of point p lies between 2 (p // 512) / 8 and 2 (p // 512 + 1) / 8; the other two lie in [0, 1].
All inputs are finite; a program needn't handle non-finite values.
Results may differ from the reference program's by a relative error of at most 0.0049.
Values may be sent and summed in bfloat16 or wider, within the bound.
A program may use at most 128 MiB of HBM per device.

```python
import jax
import jax.numpy as jnp
from jax import lax

LEAF = 512
RANK = 256
SAMP = 512
NPTS = 4096
N_NODE = 8


def draw_coords(key, part):
    unit = jax.random.uniform(key, (3, N_NODE * LEAF), jnp.float32)
    leaf_ids = (jnp.arange(N_NODE * LEAF) // LEAF).astype(jnp.float32)
    first = 2.0 * (leaf_ids + unit[0]) / N_NODE
    others = unit[1:]
    return jnp.concatenate([first[None, :], others], axis=0).astype(jnp.float32)


def draw_skeleton(key, part):
    key_one, random_key_second, key_three, key_four, key_five = jax.random.split(key, 5)
    capacity = max(8, 2 * RANK // (N_NODE - 1))
    position_count = N_NODE * capacity
    node_ids = jnp.arange(N_NODE, dtype=jnp.int32)
    popular = jax.random.randint(key_one, (), 0, N_NODE, dtype=jnp.int32)
    filled_owner = jnp.where(node_ids == popular, (popular + 1) % N_NODE, popular)
    linear_index = jnp.arange(position_count, dtype=jnp.int32).reshape(1, N_NODE, capacity)
    holder_preference = jax.random.randint(random_key_second, (N_NODE,), 0, 3, dtype=jnp.int32) * 512
    unadjusted_score = jax.random.randint(key_three, (N_NODE, N_NODE, capacity), 0, 1024, dtype=jnp.int32)
    owner_ids = node_ids[None, :, None]
    ranking_score = (unadjusted_score + holder_preference[None, :, None]) * position_count + linear_index
    ranking_score = jnp.where(owner_ids == filled_owner[:, None, None], 3000 * position_count + linear_index, ranking_score)
    ranking_score = jnp.where(owner_ids == node_ids[:, None, None], -1 - linear_index, ranking_score)
    unused, chosen = lax.top_k(ranking_score.reshape(N_NODE, position_count), RANK)
    chosen_owner = chosen // capacity
    chosen_slot = chosen % capacity
    offset_base = jax.random.randint(key_four, (N_NODE, N_NODE), 0, LEAF, dtype=jnp.int32)
    stride_step = 2 * jax.random.randint(key_five, (N_NODE, N_NODE), 0, LEAF // 2, dtype=jnp.int32) + 1
    base_taken = jnp.take_along_axis(offset_base, chosen_owner, axis=1)
    stride_taken = jnp.take_along_axis(stride_step, chosen_owner, axis=1)
    local_index = (base_taken + chosen_slot * stride_taken) % LEAF
    return (chosen_owner * LEAF + local_index).astype(jnp.int32)


def block_levels(rng, shape, shards, smallest, high):
    gain, own = 1.0, jax.random.fold_in(rng, 6)
    for dim, blocks in shards:
        heights = jnp.exp(jax.random.uniform(jax.random.fold_in(own, dim), (blocks,), jnp.float32, smallest / len(shards), high / len(shards)))
        gain = gain * jnp.repeat(heights, shape[dim] // blocks).reshape([-1 if axis == dim else 1 for axis in range(len(shape))])
    return gain


def centred(own_key, dims, deviation, most, cuts=(), held_as=jnp.bfloat16):
    entries = deviation * jax.random.normal(own_key, dims, jnp.float32)
    if cuts:
        entries = entries * block_levels(own_key, dims, cuts, -0.22, 0.18)
    return jnp.clip(entries, -most, most).astype(held_as)


def setup_inputs(seed: int = 0) -> dict:
    splits = jax.random.split(jax.random.key(seed), 4)
    return {
        "coords": draw_coords(jax.random.fold_in(splits[3], 71), 0),
        "omega": centred(splits[1], (NPTS, SAMP), 1.0, 6.0, ((0, 8), (1, 4))),
        "skeleton": draw_skeleton(jax.random.fold_in(splits[3], 71), 0),
    }


kernel_scale = 0.0078125
softening = 0.02

def kernel_tile(first_points, target_points):
    squared = (first_points[0][:, None] - target_points[0][None, :]) ** 2
    squared = squared + (first_points[1][:, None] - target_points[1][None, :]) ** 2
    squared = squared + (first_points[2][:, None] - target_points[2][None, :]) ** 2
    return (kernel_scale * lax.rsqrt(squared + softening * softening)).astype(jnp.bfloat16)

def reference(coords, omega, skeleton):
    padded_points = jnp.pad(coords, ((0, 0), (LEAF, LEAF)))
    padded_rows = jnp.pad(omega, ((LEAF, LEAF), (0, 0)))

    def advance(col_total, node_index):
        start = (node_index * LEAF).astype(jnp.int32)
        own_points = lax.dynamic_slice_in_dim(coords, start, LEAF, 1)
        own_rows = lax.dynamic_slice_in_dim(omega, start, LEAF, 0)
        wide_points = lax.dynamic_slice_in_dim(padded_points, start, 3 * LEAF, 1)
        wide_rows = lax.dynamic_slice_in_dim(padded_rows, start, 3 * LEAF, 0)
        row_total = jnp.dot(kernel_tile(own_points, wide_points), wide_rows, preferred_element_type=jnp.float32)
        listed = skeleton[node_index]
        skel_tile = kernel_tile(own_points, coords[:, listed])
        row_total = row_total + jnp.dot(skel_tile, omega[listed], preferred_element_type=jnp.float32)
        transposed = lax.dot_general(skel_tile, own_rows, (((0,), (0,)), ((), ())), preferred_element_type=jnp.float32)
        col_total = col_total.at[listed].add(transposed)
        return (col_total, row_total.astype(jnp.bfloat16))
    col_total, blocked_rows = lax.scan(advance, jnp.zeros((N_NODE * LEAF, SAMP), jnp.float32), jnp.arange(N_NODE, dtype=jnp.int32))
    return (blocked_rows.reshape(N_NODE * LEAF, SAMP), col_total)
```

```python
import functools

import jax
import jax.numpy as jnp
from jax import lax
from jax.experimental import pallas as pl
from jax.experimental.pallas import tpu as pltpu
from jax.sharding import PartitionSpec as P

kernel_scale = 0.0078125
softening = 0.02
f32, bf16 = jnp.float32, jnp.bfloat16
MESH = pl.DeviceIdType.MESH


def each(start, stop, body):
    if stop - start <= 8:
        for i in range(start, stop):
            body(i)
    else:
        lax.fori_loop(start, stop, lambda i, c: (body(i), c)[1], 0)


def far_first(n, body):
    half = n // 2
    if n <= 16:
        for d in sorted(range(1, n), key=lambda d: (abs(d - half), d)):
            body(d)
    else:
        each(0, n - 1, lambda d: body(1 + lax.rem(d + half - 1, n - 1)))


def tile(col, row):
    squared = (col[:, 0:1] - row[0:1, :]) ** 2
    squared = squared + (col[:, 1:2] - row[1:2, :]) ** 2
    squared = squared + (col[:, 2:3] - row[2:3, :]) ** 2
    return (kernel_scale * lax.rsqrt(squared + softening * softening)).astype(bf16)


def dot(a, b):
    return jnp.dot(a, b, preferred_element_type=f32)


def kernel(n, reps, cap, coords_in, omega_in, skel_in, row_out, col_out,
           coords, omega, skel, loaded, lists, points, side, keyed, local_req, local_own, rows_out, rows_in, prod_out, prod_in,
           pick_own, far_tile, total,
           list_send, list_recv, point_send, point_recv, side_send, side_recv,
           rows_send, rows_recv, prod_send, prod_recv):
    leaf = coords.shape[1]
    piece = skel.shape[1]
    rank = piece * reps
    me, my_rep = lax.axis_index("node"), lax.axis_index("rep")
    flat = me * reps + my_rep
    count = n * reps

    def at(node, rep):
        return {"node": node, "rep": rep}

    def other(d):
        t = lax.rem(flat + d, count)
        return lax.div(t, reps), lax.rem(t, reps)

    barrier = pltpu.get_barrier_semaphore()

    def greet(d):
        node, rep = other(d)
        pl.semaphore_signal(barrier, inc=1, device_id=at(node, rep), device_id_type=MESH)

    each(1, count, greet)

    loads = [pltpu.make_async_copy(a, b, loaded.at[i]) for i, (a, b) in
             enumerate(((coords_in, coords), (omega_in, omega), (skel_in, skel)))]
    for load in loads:
        load.start()
    for load in loads:
        load.wait()
    own_points = coords[...]
    own_cols = jnp.transpose(jnp.concatenate([own_points, jnp.zeros((5, leaf), f32)], axis=0))
    total[...] = dot(tile(own_cols, own_points), omega[...])
    points[me] = own_points
    lists[my_rep, pl.ds(me, 1)] = skel[...]
    rows_in[me] = jnp.zeros((cap, omega.shape[1]), bf16)
    prod_in[me] = jnp.zeros((cap, omega.shape[1]), bf16)

    pl.semaphore_wait(barrier, count - 1)

    def list_copy(d, node, rep, index):
        return pltpu.make_async_remote_copy(
            src_ref=skel, dst_ref=lists.at[my_rep, pl.ds(me, 1)],
            send_sem=list_send.at[d], recv_sem=list_recv.at[index],
            device_id=at(node, rep), device_id_type=MESH)

    def list_arrival(d):
        node, rep = other(d)
        return pltpu.make_async_remote_copy(
            src_ref=skel, dst_ref=lists.at[rep, pl.ds(node, 1)],
            send_sem=list_send.at[d], recv_sem=list_recv.at[node * reps + rep],
            device_id=at(node, rep), device_id_type=MESH)

    def start_list(d):
        node, rep = other(d)
        list_copy(d, node, rep, flat).start()

    each(1, count, start_list)

    def exchange(d, back, src, dst, send, recv):
        peer = lax.rem(me + d, n)
        place = peer if back else me
        return pltpu.make_async_remote_copy(
            src_ref=src(peer), dst_ref=dst.at[place], send_sem=send.at[peer],
            recv_sem=recv.at[place], device_id=at(peer, my_rep), device_id_type=MESH)

    point_x = lambda d, back=False: exchange(d, back, lambda peer: coords, points, point_send, point_recv)
    rows_x = lambda d, back=False: exchange(d, back, lambda peer: rows_out.at[peer], rows_in, rows_send, rows_recv)
    prod_x = lambda d, back=False: exchange(d, back, lambda peer: prod_out.at[peer], prod_in, prod_send, prod_recv)

    each(1, n, lambda d: point_x(d).start())

    def side_copy(slot):
        peer = me + (1 if slot == 0 else -1)
        return pltpu.make_async_remote_copy(
            src_ref=omega, dst_ref=side.at[slot], send_sem=side_send.at[slot],
            recv_sem=side_recv.at[slot], device_id=at(peer, my_rep), device_id_type=MESH)

    has_above, has_below = me < n - 1, me > 0

    @pl.when(has_above)
    def _():
        side_copy(0).start()

    @pl.when(has_below)
    def _():
        side_copy(1).start()

    each(1, count, lambda d: list_arrival(d).wait_recv())

    listed = jnp.concatenate([lists[r] for r in range(reps)], axis=1)
    mine = jnp.concatenate([lists[r, pl.ds(me, 1)] for r in range(reps)], axis=1)
    local_own[...] = lax.rem(listed, leaf).astype(f32)
    local_req[...] = lax.rem(mine, leaf).astype(f32)
    hit_req = lax.div(mine, leaf) == lax.broadcasted_iota(jnp.int32, (n, rank), 0)
    hit_own = lax.div(listed, leaf) == me
    before = (lax.broadcasted_iota(jnp.int32, (rank, rank), 0)
              < lax.broadcasted_iota(jnp.int32, (rank, rank), 1)).astype(f32).astype(bf16)
    keyed[0] = jnp.where(hit_req, dot(hit_req.astype(f32).astype(bf16), before), -1.0)
    keyed[1] = jnp.where(hit_own, dot(hit_own.astype(f32).astype(bf16), before), -1.0)

    slot_ids = lax.broadcasted_iota(jnp.int32, (cap, rank), 0).astype(f32)
    leaf_ids = lax.broadcasted_iota(jnp.int32, (cap, leaf), 1).astype(f32)

    def picker(keys, local):
        found = jnp.sum(jnp.where(keys == slot_ids, local + 1.0, 0.0), axis=1, keepdims=True)
        return jnp.where(found - 1.0 == leaf_ids, 1.0, 0.0).astype(bf16)

    def send_rows(d):
        peer = lax.rem(me + d, n)
        pick = picker(keyed[1, pl.ds(peer, 1)], local_own[pl.ds(peer, 1)])
        pick_own[peer] = pick
        rows_out[peer] = dot(pick, omega[...]).astype(bf16)
        rows_x(d).start()

    def send_products(d):
        peer = lax.rem(me + d, n)
        point_x(d, True).wait_recv()
        pick = picker(keyed[0, pl.ds(peer, 1)], local_req[...])
        whole = points[peer]
        high = whole.astype(bf16).astype(f32)
        middle = (whole - high).astype(bf16).astype(f32)
        low = whole - high - middle
        parts = jnp.concatenate([high, middle, low], axis=0).astype(bf16)
        got = lax.dot_general(pick, parts, (((1,), (1,)), ((), ())), preferred_element_type=f32)
        slots = got[:, 0:3] + got[:, 3:6] + got[:, 6:9]
        skel_tile = tile(slots, own_points)
        far_tile[peer] = skel_tile
        prod_out[peer] = dot(skel_tile, omega[...]).astype(bf16)
        prod_x(d).start()

    far_first(n, send_rows)
    pick_own[me] = jnp.zeros((cap, leaf), bf16)
    far_tile[me] = jnp.zeros((cap, leaf), bf16)
    far_first(n, send_products)

    @pl.when(has_below)
    def _():
        side_copy(0).wait_recv()
        total[...] += dot(tile(own_cols, points[jnp.maximum(me - 1, 0)]), side[0])

    @pl.when(has_above)
    def _():
        side_copy(1).wait_recv()
        total[...] += dot(tile(own_cols, points[jnp.minimum(me + 1, n - 1)]), side[1])

    far = far_tile[...].reshape(n * cap, leaf).T
    back = pick_own[...].reshape(n * cap, leaf).T

    each(1, n, lambda d: rows_x(d, True).wait_recv())
    row_out[...] = (total[...] + dot(far, rows_in[...].reshape(n * cap, -1)))
    each(1, n, lambda d: prod_x(d, True).wait_recv())
    col_out[...] = dot(back, prod_in[...].reshape(n * cap, -1))

    each(1, count, lambda d: list_arrival(d).wait_send())
    each(1, n, lambda d: point_x(d).wait_send())
    each(1, n, lambda d: rows_x(d).wait_send())
    each(1, n, lambda d: prod_x(d).wait_send())

    @pl.when(has_above)
    def _():
        side_copy(0).wait_send()

    @pl.when(has_below)
    def _():
        side_copy(1).wait_send()


def near_kernel(n, reps, cap, sent, coords_in, omega_in, skel_in, row_out, col_out,
                coords, omega, skel, lists, points, side, rows_out, rows_in, prod_out,
                prod_in, pick_own, pick_req, far_tile, total,
                loaded, piece_send, piece_recv, list_send, list_recv, point_send, point_recv,
                side_send, side_recv, rows_send, rows_recv, prod_send, prod_recv, above, below):
    leaf, samp = omega.shape
    rank = skel.shape[1] * reps
    me, my_rep = lax.axis_index("node"), lax.axis_index("rep")
    close = (-2, -1, 1, 2)
    distant = [o * sign for o in sorted(range(3, n), key=lambda o: abs(o - n // 2)) for sign in (1, -1)]
    place = {o: k for k, o in enumerate(close)}

    def if_there(offset, body):
        @pl.when(me + offset < n if offset > 0 else me + offset >= 0)
        def _():
            body()

    def signal(sem, node, rep):
        pl.semaphore_signal(sem, inc=1, device_id={"node": node, "rep": rep}, device_id_type=MESH)

    def send(src, dst, send_sem, recv_sem, node, rep):
        return pltpu.make_async_remote_copy(
            src_ref=src, dst_ref=dst, send_sem=send_sem, recv_sem=recv_sem,
            device_id={"node": node, "rep": rep}, device_id_type=MESH)

    def exchange(offset, back, src, dst, send_sems, recv_sems):
        peer = me + offset
        spot = peer if back else me
        return send(src(peer), dst(spot), send_sems.at[peer], recv_sems.at[spot], peer, my_rep)

    def point_x(o, back=False):
        return exchange(o, back, lambda p: coords, lambda p: points.at[p], point_send, point_recv)

    def list_x(o, k, back=False):
        rep, peer = lax.rem(my_rep + k, reps), me + o
        spot = peer if back else me
        return send(lists.at[rep, pl.ds(me, 1)] if k else skel, lists.at[rep, pl.ds(spot, 1)],
                    list_send.at[peer, rep], list_recv.at[spot, rep], peer, my_rep)

    def rows_x(o, back=False):
        return exchange(o, back, lambda p: rows_out.at[p, pl.ds(0, sent)], lambda p: rows_in.at[p, pl.ds(0, sent)], rows_send, rows_recv)

    def prod_x(o, back=False):
        return exchange(o, back, lambda p: prod_out.at[p, pl.ds(0, sent)], lambda p: prod_in.at[p, pl.ds(0, sent)], prod_send, prod_recv)

    def piece_x(k, back=False):
        rep = lax.rem(my_rep + k, reps)
        spot = rep if back else my_rep
        return send(skel, lists.at[spot, pl.ds(me, 1)], piece_send.at[rep], piece_recv.at[spot], me, rep)

    def side_x(o, back=False):
        spot = place[o] if back else place[-o]
        return send(omega, side.at[spot], side_send.at[place[o]], side_recv.at[spot], me + o, my_rep)

    barrier = pltpu.get_barrier_semaphore()
    for k in range(1, reps):
        signal(barrier, me, lax.rem(my_rep + k, reps))
    for o in close:
        if_there(o, lambda o=o: signal(barrier, me + o, my_rep))

    loads = [pltpu.make_async_copy(a, b, loaded.at[i]) for i, (a, b) in
             enumerate(((coords_in, coords), (omega_in, omega), (skel_in, skel)))]
    for load in loads:
        load.start()
    for load in loads:
        load.wait()
    own_points = coords[...]
    own_cols = jnp.transpose(jnp.concatenate([own_points, jnp.zeros((5, leaf), f32)], axis=0))
    points[me] = own_points
    lists[my_rep, pl.ds(me, 1)] = skel[...]
    rows_in[...] = jnp.zeros((n, cap, samp), bf16)
    prod_in[...] = jnp.zeros((n, cap, samp), bf16)

    edge = me * (n - 1 - me)
    for met, level in ((2, edge == 0), (3, edge == n - 2), (4, edge > n - 2)):
        @pl.when(level)
        def _():
            pl.semaphore_wait(barrier, reps - 1 + met)

    for k in range(1, reps):
        piece_x(k).start()
    for sign, sem in ((1, above), (-1, below)):
        def first(sign=sign, sem=sem):
            if_there(-2 * sign, lambda: signal(sem, me - 2 * sign, my_rep))
        if_there(sign, first)
    for o in close:
        if_there(o, lambda o=o: point_x(o).start())
    even = lax.rem(me, 2) == 0
    for o in (-2, 2):
        if_there(o, lambda o=o: side_x(o).start())
    for o in (-1, 1):
        @pl.when(even if o == 1 else jnp.logical_not(even))
        def _():
            if_there(o, lambda: side_x(o).start())
    for s in range(2, n // 2 + 1):
        for sign, sem in ((1, above), (-1, below)):
            def hop(s=s, sign=sign, sem=sem):
                pl.semaphore_wait(sem, 1)
                if_there(-2 * sign, lambda: signal(sem, me - 2 * sign, my_rep))
            if_there(sign * (2 * s - 1), hop)

    for k in range(1, reps):
        piece_x(k, True).wait_recv()
    for o in distant + list(close):
        def lists_out(o=o):
            for k in range(reps):
                list_x(o, k).start()
        if_there(o, lists_out)
    for o in distant:
        if_there(o, lambda o=o: point_x(o).start())
    for o in (-1, 1):
        @pl.when(even if o == -1 else jnp.logical_not(even))
        def _():
            if_there(o, lambda: side_x(o).start())
    total[...] = dot(tile(own_cols, own_points), omega[...])
    for o in distant + list(close):
        def lists_in(o=o):
            for k in range(reps):
                list_x(o, k, True).wait_recv()
        if_there(o, lists_in)

    listed = jnp.concatenate([lists[r] for r in range(reps)], axis=1)
    mine = jnp.concatenate([lists[r, pl.ds(me, 1)] for r in range(reps)], axis=1)
    local_own = lax.rem(listed, leaf).astype(f32)
    local_req = lax.rem(mine, leaf).astype(f32)
    hit_req = lax.div(mine, leaf) == lax.broadcasted_iota(jnp.int32, (n, rank), 0)
    hit_own = lax.div(listed, leaf) == me
    before = (lax.broadcasted_iota(jnp.int32, (rank, rank), 0)
              < lax.broadcasted_iota(jnp.int32, (rank, rank), 1)).astype(f32).astype(bf16)
    key_req = jnp.where(hit_req, dot(hit_req.astype(f32).astype(bf16), before), -1.0)
    key_own = jnp.where(hit_own, dot(hit_own.astype(f32).astype(bf16), before), -1.0)
    slot_ids = lax.broadcasted_iota(jnp.int32, (cap, rank), 0).astype(f32)
    leaf_ids = lax.broadcasted_iota(jnp.int32, (cap, leaf), 1).astype(f32)

    def picker(keys, local):
        found = jnp.sum(jnp.where(keys == slot_ids, local + 1.0, 0.0), axis=1, keepdims=True)
        return jnp.where(found - 1.0 == leaf_ids, 1.0, 0.0).astype(bf16)

    def places(pick, whole):
        high = whole.astype(bf16).astype(f32)
        middle = (whole - high).astype(bf16).astype(f32)
        low = whole - high - middle
        parts = jnp.concatenate([high, middle, low], axis=0).astype(bf16)
        got = lax.dot_general(pick, parts, (((1,), (1,)), ((), ())), preferred_element_type=f32)
        return got[:, 0:3] + got[:, 3:6] + got[:, 6:9]

    for i in range(n):
        pick = picker(key_own[i:i + 1], local_own[i:i + 1])
        pick_own[i] = pick
        rows_out[i] = dot(pick, omega[...]).astype(bf16)
    for o in distant:
        if_there(o, lambda o=o: rows_x(o).start())
    for o in distant + list(close):
        if_there(o, lambda o=o: point_x(o, True).wait_recv())
    for j in range(n):
        pick = picker(key_req[j:j + 1], local_req)
        pick_req[j] = pick
        skel_tile = tile(places(pick, points[j]), own_points)
        far_tile[j] = skel_tile
        prod_out[j] = dot(skel_tile, omega[...]).astype(bf16)
    for o in distant:
        if_there(o, lambda o=o: prod_x(o).start())

    def from_side(o):
        peer = me + o
        side_x(o, True).wait_recv()
        rows = side[place[o]]
        rows_in[peer] = dot(pick_req[peer], rows).astype(bf16)
        there = points[peer]
        prod_in[peer] = dot(tile(places(pick_own[peer], own_points), there), rows).astype(bf16)
        if abs(o) == 1:
            total[...] += dot(tile(own_cols, there), rows)

    for o in (-2, 2, -1, 1):
        if_there(o, lambda o=o: from_side(o))

    far = far_tile[...].reshape(n * cap, leaf).T
    back = pick_own[...].reshape(n * cap, leaf).T
    for o in distant:
        if_there(o, lambda o=o: rows_x(o, True).wait_recv())
    row_out[...] = total[...] + dot(far, rows_in[...].reshape(n * cap, samp))
    for o in distant:
        if_there(o, lambda o=o: prod_x(o, True).wait_recv())
    col_out[...] = dot(back, prod_in[...].reshape(n * cap, samp))

    for k in range(1, reps):
        piece_x(k).wait_send()
    for o in distant:
        def done(o=o):
            for x in (point_x, rows_x, prod_x):
                x(o).wait_send()
            for k in range(reps):
                list_x(o, k).wait_send()
        if_there(o, done)
    for o in close:
        def done(o=o):
            for x in (point_x, side_x):
                x(o).wait_send()
            for k in range(reps):
                list_x(o, k).wait_send()
        if_there(o, done)


def near_call(n, reps, cap, coords, omega, skeleton):
    leaf, samp = omega.shape
    piece = skeleton.shape[1]
    need = max(8, 2 * piece * reps // (n - 1))
    sent = need + need % 2
    vmem = pl.BlockSpec(memory_space=pltpu.VMEM)
    sem = pltpu.SemaphoreType.DMA
    return pl.pallas_call(
        functools.partial(near_kernel, n, reps, cap, sent),
        out_shape=(pltpu.VMEM((leaf, samp), f32), pltpu.VMEM((leaf, samp), f32)),
        in_specs=[pl.BlockSpec(memory_space=pltpu.HBM)] * 3,
        out_specs=(vmem, vmem),
        scratch_shapes=[
            pltpu.VMEM(coords.shape, f32),
            pltpu.VMEM(omega.shape, bf16),
            pltpu.VMEM(skeleton.shape, jnp.int32),
            pltpu.VMEM((reps, n, piece), jnp.int32),
            pltpu.VMEM((n, 3, leaf), f32),
            pltpu.VMEM((4, leaf, samp), bf16),
            pltpu.VMEM((n, cap, samp), bf16),
            pltpu.VMEM((n, cap, samp), bf16),
            pltpu.VMEM((n, cap, samp), bf16),
            pltpu.VMEM((n, cap, samp), bf16),
            pltpu.VMEM((n, cap, leaf), bf16),
            pltpu.VMEM((n, cap, leaf), bf16),
            pltpu.VMEM((n, cap, leaf), bf16),
            pltpu.VMEM((leaf, samp), f32),
            sem((3,)), sem((reps,)), sem((reps,)),
            sem((n, reps)), sem((n, reps)), sem((n,)), sem((n,)), sem((4,)), sem((4,)),
            sem((n,)), sem((n,)), sem((n,)), sem((n,)),
            pltpu.SemaphoreType.REGULAR, pltpu.SemaphoreType.REGULAR,
        ],
        compiler_params=pltpu.CompilerParams(collective_id=0, has_side_effects=True),
    )(coords, omega, skeleton)


def finish_kernel(row, col, row_out, col_out):
    row_out[...] = row[...].astype(bf16)
    col_out[...] = col[...]


def finish(row, col):
    vmem = pl.BlockSpec(memory_space=pltpu.VMEM)
    return pl.pallas_call(
        finish_kernel,
        out_shape=(jax.ShapeDtypeStruct(row.shape, bf16), jax.ShapeDtypeStruct(col.shape, f32)),
        in_specs=[vmem] * 2, out_specs=(vmem, vmem),
        compiler_params=pltpu.CompilerParams(vmem_limit_bytes=16 << 20))(row, col)


def on_device(n, reps, coords, omega, skeleton):
    leaf, samp = omega.shape
    piece = skeleton.shape[1]
    rank = piece * reps
    cap = -(-max(8, 2 * rank // (n - 1)) // 16) * 16
    if 6 <= n <= 16:
        return finish(*near_call(n, reps, cap, coords, omega, skeleton))
    vmem = pl.BlockSpec(memory_space=pltpu.VMEM)
    sem = pltpu.SemaphoreType.DMA
    row, col = pl.pallas_call(
        functools.partial(kernel, n, reps, cap),
        out_shape=(jax.ShapeDtypeStruct((leaf, samp), f32), jax.ShapeDtypeStruct((leaf, samp), f32)),
        in_specs=[pl.BlockSpec(memory_space=pl.ANY)] * 3,
        out_specs=(vmem, vmem),
        scratch_shapes=[
            pltpu.VMEM(coords.shape, f32),
            pltpu.VMEM(omega.shape, bf16),
            pltpu.VMEM(skeleton.shape, jnp.int32),
            sem((3,)),
            pltpu.VMEM((reps, n, piece), jnp.int32),
            pltpu.VMEM((n, 3, leaf), f32),
            pltpu.VMEM((2, leaf, samp), bf16),
            pltpu.VMEM((2, n, rank), f32),
            pltpu.VMEM((1, rank), f32),
            pltpu.VMEM((n, rank), f32),
            pltpu.VMEM((n, cap, samp), bf16),
            pltpu.VMEM((n, cap, samp), bf16),
            pltpu.VMEM((n, cap, samp), bf16),
            pltpu.VMEM((n, cap, samp), bf16),
            pltpu.VMEM((n, cap, leaf), bf16),
            pltpu.VMEM((n, cap, leaf), bf16),
            pltpu.VMEM((leaf, samp), f32),
            sem((n * reps,)), sem((n * reps,)),
            sem((n,)), sem((n,)), sem((2,)), sem((2,)),
            sem((n,)), sem((n,)), sem((n,)), sem((n,)),
        ],
        compiler_params=pltpu.CompilerParams(collective_id=0, has_side_effects=True),
    )(coords, omega, skeleton)
    return finish(row, col)


def solution(mesh):
    in_specs = (P(None, "node"), P("node", "rep"), P("node", "rep"))
    out_specs = (P("node", "rep"), P("node", "rep"))
    body = functools.partial(on_device, mesh.shape["node"], mesh.shape["rep"])
    return jax.shard_map(body, mesh=mesh, in_specs=in_specs, out_specs=out_specs, check_vma=False)
```

```python
import functools

import jax
import jax.numpy as jnp
from jax import lax
from jax.experimental import pallas as pl
from jax.experimental.pallas import tpu as pltpu
from jax.sharding import PartitionSpec as P

kernel_scale = 0.0078125
softening = 0.02
f32, bf16 = jnp.float32, jnp.bfloat16
MESH = pl.DeviceIdType.MESH


def each(start, stop, body):
    if stop - start <= 8:
        for i in range(start, stop):
            body(i)
    else:
        lax.fori_loop(start, stop, lambda i, c: (body(i), c)[1], 0)


def far_first(n, body):
    half = n // 2
    if n <= 16:
        for d in sorted(range(1, n), key=lambda d: (abs(d - half), d)):
            body(d)
    else:
        each(0, n - 1, lambda d: body(1 + lax.rem(d + half - 1, n - 1)))


def tile(col, row, scale=kernel_scale):
    squared = (col[:, 0:1] - row[0:1, :]) ** 2
    squared = squared + (col[:, 1:2] - row[1:2, :]) ** 2
    squared = squared + (col[:, 2:3] - row[2:3, :]) ** 2
    return (scale * lax.rsqrt(squared + softening * softening)).astype(bf16)


def dot(a, b):
    return jnp.dot(a, b, preferred_element_type=f32)


def kernel(n, reps, cap, coords_in, omega_in, skel_in, row_out, col_out,
           coords, omega, skel, loaded, lists, points, side, keyed, local_req, local_own, rows_out, rows_in, prod_out, prod_in,
           pick_own, far_tile, total,
           list_send, list_recv, point_send, point_recv, side_send, side_recv,
           rows_send, rows_recv, prod_send, prod_recv):
    leaf = coords.shape[1]
    piece = skel.shape[1]
    rank = piece * reps
    me, my_rep = lax.axis_index("node"), lax.axis_index("rep")
    flat = me * reps + my_rep
    count = n * reps

    def at(node, rep):
        return {"node": node, "rep": rep}

    def other(d):
        t = lax.rem(flat + d, count)
        return lax.div(t, reps), lax.rem(t, reps)

    barrier = pltpu.get_barrier_semaphore()

    def greet(d):
        node, rep = other(d)
        pl.semaphore_signal(barrier, inc=1, device_id=at(node, rep), device_id_type=MESH)

    each(1, count, greet)

    loads = [pltpu.make_async_copy(a, b, loaded.at[i]) for i, (a, b) in
             enumerate(((coords_in, coords), (omega_in, omega), (skel_in, skel)))]
    for load in loads:
        load.start()
    for load in loads:
        load.wait()
    own_points = coords[...]
    own_cols = jnp.transpose(jnp.concatenate([own_points, jnp.zeros((5, leaf), f32)], axis=0))
    total[...] = dot(tile(own_cols, own_points), omega[...])
    points[me] = own_points
    lists[my_rep, pl.ds(me, 1)] = skel[...]
    rows_in[me] = jnp.zeros((cap, omega.shape[1]), bf16)
    prod_in[me] = jnp.zeros((cap, omega.shape[1]), bf16)

    pl.semaphore_wait(barrier, count - 1)

    def list_copy(d, node, rep, index):
        return pltpu.make_async_remote_copy(
            src_ref=skel, dst_ref=lists.at[my_rep, pl.ds(me, 1)],
            send_sem=list_send.at[d], recv_sem=list_recv.at[index],
            device_id=at(node, rep), device_id_type=MESH)

    def list_arrival(d):
        node, rep = other(d)
        return pltpu.make_async_remote_copy(
            src_ref=skel, dst_ref=lists.at[rep, pl.ds(node, 1)],
            send_sem=list_send.at[d], recv_sem=list_recv.at[node * reps + rep],
            device_id=at(node, rep), device_id_type=MESH)

    def start_list(d):
        node, rep = other(d)
        list_copy(d, node, rep, flat).start()

    each(1, count, start_list)

    def exchange(d, back, src, dst, send, recv):
        peer = lax.rem(me + d, n)
        place = peer if back else me
        return pltpu.make_async_remote_copy(
            src_ref=src(peer), dst_ref=dst.at[place], send_sem=send.at[peer],
            recv_sem=recv.at[place], device_id=at(peer, my_rep), device_id_type=MESH)

    point_x = lambda d, back=False: exchange(d, back, lambda peer: coords, points, point_send, point_recv)
    rows_x = lambda d, back=False: exchange(d, back, lambda peer: rows_out.at[peer], rows_in, rows_send, rows_recv)
    prod_x = lambda d, back=False: exchange(d, back, lambda peer: prod_out.at[peer], prod_in, prod_send, prod_recv)

    each(1, n, lambda d: point_x(d).start())

    def side_copy(slot):
        peer = me + (1 if slot == 0 else -1)
        return pltpu.make_async_remote_copy(
            src_ref=omega, dst_ref=side.at[slot], send_sem=side_send.at[slot],
            recv_sem=side_recv.at[slot], device_id=at(peer, my_rep), device_id_type=MESH)

    has_above, has_below = me < n - 1, me > 0

    @pl.when(has_above)
    def _():
        side_copy(0).start()

    @pl.when(has_below)
    def _():
        side_copy(1).start()

    each(1, count, lambda d: list_arrival(d).wait_recv())

    listed = jnp.concatenate([lists[r] for r in range(reps)], axis=1)
    mine = jnp.concatenate([lists[r, pl.ds(me, 1)] for r in range(reps)], axis=1)
    local_own[...] = lax.rem(listed, leaf).astype(f32)
    local_req[...] = lax.rem(mine, leaf).astype(f32)
    hit_req = lax.div(mine, leaf) == lax.broadcasted_iota(jnp.int32, (n, rank), 0)
    hit_own = lax.div(listed, leaf) == me
    before = (lax.broadcasted_iota(jnp.int32, (rank, rank), 0)
              < lax.broadcasted_iota(jnp.int32, (rank, rank), 1)).astype(f32).astype(bf16)
    keyed[0] = jnp.where(hit_req, dot(hit_req.astype(f32).astype(bf16), before), -1.0)
    keyed[1] = jnp.where(hit_own, dot(hit_own.astype(f32).astype(bf16), before), -1.0)

    slot_ids = lax.broadcasted_iota(jnp.int32, (cap, rank), 0).astype(f32)
    leaf_ids = lax.broadcasted_iota(jnp.int32, (cap, leaf), 1).astype(f32)

    def picker(keys, local):
        found = jnp.sum(jnp.where(keys == slot_ids, local + 1.0, 0.0), axis=1, keepdims=True)
        return jnp.where(found - 1.0 == leaf_ids, 1.0, 0.0).astype(bf16)

    def send_rows(d):
        peer = lax.rem(me + d, n)
        pick = picker(keyed[1, pl.ds(peer, 1)], local_own[pl.ds(peer, 1)])
        pick_own[peer] = pick
        rows_out[peer] = dot(pick, omega[...]).astype(bf16)
        rows_x(d).start()

    def send_products(d):
        peer = lax.rem(me + d, n)
        point_x(d, True).wait_recv()
        pick = picker(keyed[0, pl.ds(peer, 1)], local_req[...])
        whole = points[peer]
        high = whole.astype(bf16).astype(f32)
        middle = (whole - high).astype(bf16).astype(f32)
        low = whole - high - middle
        parts = jnp.concatenate([high, middle, low], axis=0).astype(bf16)
        got = lax.dot_general(pick, parts, (((1,), (1,)), ((), ())), preferred_element_type=f32)
        slots = got[:, 0:3] + got[:, 3:6] + got[:, 6:9]
        skel_tile = tile(slots, own_points)
        far_tile[peer] = skel_tile
        prod_out[peer] = dot(skel_tile, omega[...]).astype(bf16)
        prod_x(d).start()

    far_first(n, send_rows)
    pick_own[me] = jnp.zeros((cap, leaf), bf16)
    far_tile[me] = jnp.zeros((cap, leaf), bf16)
    far_first(n, send_products)

    @pl.when(has_below)
    def _():
        side_copy(0).wait_recv()
        total[...] += dot(tile(own_cols, points[jnp.maximum(me - 1, 0)]), side[0])

    @pl.when(has_above)
    def _():
        side_copy(1).wait_recv()
        total[...] += dot(tile(own_cols, points[jnp.minimum(me + 1, n - 1)]), side[1])

    far = far_tile[...].reshape(n * cap, leaf).T
    back = pick_own[...].reshape(n * cap, leaf).T

    each(1, n, lambda d: rows_x(d, True).wait_recv())
    row_out[...] = (total[...] + dot(far, rows_in[...].reshape(n * cap, -1)))
    each(1, n, lambda d: prod_x(d, True).wait_recv())
    col_out[...] = dot(back, prod_in[...].reshape(n * cap, -1))

    each(1, count, lambda d: list_arrival(d).wait_send())
    each(1, n, lambda d: point_x(d).wait_send())
    each(1, n, lambda d: rows_x(d).wait_send())
    each(1, n, lambda d: prod_x(d).wait_send())

    @pl.when(has_above)
    def _():
        side_copy(0).wait_send()

    @pl.when(has_below)
    def _():
        side_copy(1).wait_send()


def near_kernel(n, reps, cap, sent, coords_in, omega_in, skel_in, row_out, col_out,
                coords, omega, skel, pieces, code_out, code_in, points, side, rows_out, rows_in, prod_out,
                prod_in, pick_own, pick_req, far_tile, near_tile, edge_tile, edge_prod, total,
                loaded, piece_send, piece_recv, point_send, point_recv, code_send, code_recv,
                side_send, side_recv, rows_send, rows_recv, prod_send, prod_recv, ready):
    leaf, samp = omega.shape
    rank = skel.shape[1] * reps
    me, my_rep = lax.axis_index("node"), lax.axis_index("rep")
    first, last = (n - me) // n, (me + 1) // n
    edge = first + last
    beside = (1, -1)
    parts, slots = side_send.shape[1], n - 2
    late = range(3, n)

    def peer_of(k):
        before_me = (me + n - k - 2) // n
        return before_me * k + (1 - before_me) * (3 + k - first)

    peers = [peer_of(k) for k in range(n - 3)]
    peers.append(edge * peer_of(n - 3) + (1 - edge) * me)

    def if_edge(body):
        @pl.when(edge == 1)
        def _():
            body()

    def if_there(offset, body):
        @pl.when(me + offset < n if offset > 0 else me + offset >= 0)
        def _():
            body()

    def signal(sem, node, rep):
        pl.semaphore_signal(sem, inc=1, device_id={"node": node, "rep": rep}, device_id_type=MESH)

    def send(src, dst, send_sem, recv_sem, node, rep):
        return pltpu.make_async_remote_copy(
            src_ref=src, dst_ref=dst, send_sem=send_sem, recv_sem=recv_sem,
            device_id={"node": node, "rep": rep}, device_id_type=MESH)

    def exchange(peer, back, src, dst, send_sems, recv_sems):
        spot = peer if back else me
        return send(src(peer), dst(spot), send_sems.at[peer], recv_sems.at[spot], peer, my_rep)

    def point_x(peer, back=False):
        return exchange(peer, back, lambda p: coords, lambda p: points.at[p], point_send, point_recv)

    def code_x(peer, back=False):
        return exchange(peer, back, lambda p: code_out.at[p], lambda p: code_in.at[p], code_send, code_recv)

    def rows_x(peer, back=False):
        return exchange(peer, back, lambda p: rows_out.at[p, pl.ds(0, sent)], lambda p: rows_in.at[p, pl.ds(0, sent)], rows_send, rows_recv)

    def prod_x(peer, back=False):
        return exchange(peer, back, lambda p: prod_out.at[p, pl.ds(0, sent)], lambda p: prod_in.at[p, pl.ds(0, sent)], prod_send, prod_recv)

    def side_x(slot, part, back=False):
        spot = slot if back else 1 - slot
        rows = pl.ds(part * (leaf // parts), leaf // parts)
        return send(omega.at[rows], side.at[spot, rows], side_send.at[slot, part], side_recv.at[spot, part], me + beside[slot], my_rep)

    def piece_x(k, back=False):
        rep = lax.rem(my_rep + k, reps)
        spot = rep if back else my_rep
        return send(skel, pieces.at[spot], piece_send.at[rep], piece_recv.at[spot], me, rep)

    barrier = pltpu.get_barrier_semaphore()
    for k in range(1, reps):
        signal(barrier, me, lax.rem(my_rep + k, reps))
    for o in (-1, -2, *range(1, n)):
        if_there(o, lambda o=o: signal(barrier, me + o, my_rep))

    loads = [pltpu.make_async_copy(a, b, loaded.at[i]) for i, (a, b) in
             enumerate(((skel_in, skel), (coords_in, coords), (omega_in, omega)))]
    for load in loads:
        load.start()
    for load in loads:
        load.wait()
    own_points = coords[...]
    own_cols = jnp.transpose(jnp.concatenate([own_points, jnp.zeros((5, leaf), f32)], axis=0))
    pieces[my_rep] = skel[...]
    rows_in[...] = jnp.zeros((n, cap, samp), bf16)
    prod_in[...] = jnp.zeros((n, cap, samp), bf16)
    edge_prod[...] = jnp.zeros((2, cap, samp), bf16)
    far_tile[slots - 1] = jnp.zeros((cap, leaf), bf16)
    for k in range(slots - 1, n):
        pick_own[k] = jnp.zeros((cap, leaf), bf16)

    def push(part):
        for slot in (0, 1):
            if_there(beside[slot], lambda slot=slot: side_x(slot, part).start())

    with jax.named_scope("enter"):
        pl.semaphore_wait(barrier, reps + 1 + me - last - (me + 2) // n)

    for k in range(1, reps):
        piece_x(k).start()
    for o in late:
        if_there(-o, lambda o=o: signal(ready.at[me], me - o, my_rep))
    known = (1, 2, *range(-1, -n, -1))
    for o in known:
        if_there(o, lambda o=o: point_x(me + o).start())
    push(0)

    with jax.named_scope("own"):
        total[...] = dot(tile(own_cols, own_points), omega[...])

    with jax.named_scope("pieces"):
        for k in range(1, reps):
            piece_x(k, True).wait_recv()
    mine = jnp.concatenate([pieces[r] for r in range(reps)], axis=1)
    local = lax.rem(mine, leaf).astype(f32)
    before = (lax.broadcasted_iota(jnp.int32, (rank, rank), 0)
              < lax.broadcasted_iota(jnp.int32, (rank, rank), 1)).astype(f32).astype(bf16)
    hit = lax.div(mine, leaf) == lax.broadcasted_iota(jnp.int32, (n, rank), 0)
    keys = jnp.where(hit, dot(hit.astype(f32).astype(bf16), before), -1.0)
    codes = jnp.where(hit, (keys + 1.0) * leaf + local, 0.0).astype(jnp.int32)
    for i in range(n):
        code_out[i] = codes[i:i + 1]
    for o in known:
        if_there(o, lambda o=o: code_x(me + o).start())

    for o in late:
        def follow(o=o):
            with jax.named_scope(f"ready{o}"):
                pl.semaphore_wait(ready.at[me + o], 1)
            point_x(me + o).start()
            code_x(me + o).start()
        if_there(o, follow)
    push(1)

    slot_ids = lax.broadcasted_iota(jnp.int32, (cap, rank), 0).astype(f32)
    leaf_ids = lax.broadcasted_iota(jnp.int32, (cap, leaf), 1).astype(f32)

    def picker(key, index):
        found = jnp.sum(jnp.where(key == slot_ids, index + 1.0, 0.0), axis=1, keepdims=True)
        return jnp.where(found - 1.0 == leaf_ids, 1.0, 0.0).astype(bf16)

    def places(pick, whole):
        high = whole.astype(bf16).astype(f32)
        middle = (whole - high).astype(bf16).astype(f32)
        low = whole - high - middle
        parts = jnp.concatenate([high, middle, low], axis=0).astype(bf16)
        got = lax.dot_general(pick, parts, (((1,), (1,)), ((), ())), preferred_element_type=f32)
        return got[:, 0:3] + got[:, 3:6] + got[:, 6:9]

    def asked(peer):
        code = code_in[peer]
        return picker((lax.div(code, leaf) - 1).astype(f32), lax.rem(code, leaf).astype(f32))

    with jax.named_scope("requests"):
        for i in range(n):
            pick_req[i] = picker(keys[i:i + 1], local)

    def serve(group):
        with jax.named_scope("wait" + "".join(map(str, group))):
            for k in group:
                point_x(peers[k], True).wait_recv()
                code_x(peers[k], True).wait_recv()
        with jax.named_scope("serve" + "".join(map(str, group))):
            picks = [asked(peers[k]) for k in group]
            tiles = [tile(places(pick_req[peers[k]], points[peers[k]]), own_points) for k in group]
            for k, pick in zip(group, picks):
                pick_own[k] = pick
                rows_out[peers[k]] = dot(pick, omega[...]).astype(bf16)
            for k, skel_tile in zip(group, tiles):
                far_tile[k] = skel_tile
                prod_out[peers[k]] = dot(skel_tile, omega[...]).astype(bf16)
        for k in group:
            rows_x(peers[k]).start()
            prod_x(peers[k]).start()

    for k in range(0, n - 3, 2):
        serve(list(range(k, min(k + 2, n - 3))))
    if_edge(lambda: serve([n - 3]))

    def prepare(slot):
        peer = me + beside[slot]
        with jax.named_scope(f"besidewait{slot}"):
            point_x(peer, True).wait_recv()
            code_x(peer, True).wait_recv()
        with jax.named_scope(f"beside{slot}"):
            there = points[peer]
            counted = jnp.sum(pick_req[peer].astype(f32), axis=0, keepdims=True) + 1.0
            near_tile[slot] = tile(own_cols, there, kernel_scale * counted)
            pick = asked(peer)
            pick_own[slots + slot] = pick
            edge_tile[slot] = tile(places(pick, own_points), there)

    def collect(slot):
        with jax.named_scope(f"side{slot}"):
            for part in range(parts):
                side_x(slot, part, True).wait_recv()
        with jax.named_scope(f"near{slot}"):
            edge_prod[slot] = dot(edge_tile[slot], side[slot]).astype(bf16)
            total[...] += dot(near_tile[slot], side[slot])

    for slot in (0, 1):
        if_there(beside[slot], lambda slot=slot: prepare(slot))

    with jax.named_scope("turn"):
        far = far_tile[...].reshape(slots * cap, leaf).T
        back = pick_own[...].reshape(n * cap, leaf).T

    with jax.named_scope("sent"):
        for k in range(1, reps):
            piece_x(k).wait_send()
        for o in range(1, n):
            peer = lax.rem(me + o, n)
            point_x(peer).wait_send()
            code_x(peer).wait_send()

    for slot in (0, 1):
        if_there(beside[slot], lambda slot=slot: collect(slot))

    def gather(x, name):
        for k in range(n - 3):
            with jax.named_scope(f"{name}{k}"):
                x(peers[k], True).wait_recv()

        def more():
            with jax.named_scope(f"{name}{n - 3}"):
                x(peers[n - 3], True).wait_recv()
        if_edge(more)

    gather(rows_x, "rows")
    with jax.named_scope("rowsum"):
        row_out[...] = total[...] + dot(far, jnp.concatenate([rows_in[p] for p in peers], axis=0))
    gather(prod_x, "prod")
    with jax.named_scope("colsum"):
        col_out[...] = dot(back, jnp.concatenate([prod_in[p] for p in peers] + [edge_prod[0], edge_prod[1]], axis=0))

    with jax.named_scope("sent2"):
        for slot in (0, 1):
            def sent_side(slot=slot):
                for part in range(parts):
                    side_x(slot, part).wait_send()
            if_there(beside[slot], sent_side)
        for peer in peers[:-1]:
            rows_x(peer).wait_send()
            prod_x(peer).wait_send()

        def rest():
            rows_x(peers[-1]).wait_send()
            prod_x(peers[-1]).wait_send()
        if_edge(rest)


def near_call(n, reps, cap, coords, omega, skeleton):
    leaf, samp = omega.shape
    piece = skeleton.shape[1]
    need = max(8, 2 * piece * reps // (n - 1))
    sent = need + need % 2
    vmem = pl.BlockSpec(memory_space=pltpu.VMEM)
    sem = pltpu.SemaphoreType.DMA
    return pl.pallas_call(
        functools.partial(near_kernel, n, reps, cap, sent),
        out_shape=(pltpu.VMEM((leaf, samp), f32), pltpu.VMEM((leaf, samp), f32)),
        in_specs=[pl.BlockSpec(memory_space=pltpu.HBM)] * 3,
        out_specs=(vmem, vmem),
        scratch_shapes=[
            pltpu.VMEM(coords.shape, f32),
            pltpu.VMEM(omega.shape, bf16),
            pltpu.VMEM(skeleton.shape, jnp.int32),
            pltpu.VMEM((reps, 1, piece), jnp.int32),
            pltpu.VMEM((n, 1, piece * reps), jnp.int32),
            pltpu.VMEM((n, 1, piece * reps), jnp.int32),
            pltpu.VMEM((n, 3, leaf), f32),
            pltpu.VMEM((2, leaf, samp), bf16),
            pltpu.VMEM((n, cap, samp), bf16),
            pltpu.VMEM((n, cap, samp), bf16),
            pltpu.VMEM((n, cap, samp), bf16),
            pltpu.VMEM((n, cap, samp), bf16),
            pltpu.VMEM((n, cap, leaf), bf16),
            pltpu.VMEM((n, cap, leaf), bf16),
            pltpu.VMEM((n - 2, cap, leaf), bf16),
            pltpu.VMEM((2, leaf, leaf), bf16),
            pltpu.VMEM((2, cap, leaf), bf16),
            pltpu.VMEM((2, cap, samp), bf16),
            pltpu.VMEM((leaf, samp), f32),
            sem((3,)), sem((reps,)), sem((reps,)),
            sem((n,)), sem((n,)), sem((n,)), sem((n,)), sem((2, 2)), sem((2, 2)),
            sem((n,)), sem((n,)), sem((n,)), sem((n,)),
            pltpu.SemaphoreType.REGULAR((n,)),
        ],
        compiler_params=pltpu.CompilerParams(collective_id=0, has_side_effects=True),
    )(coords, omega, skeleton)


def finish_kernel(row, col, row_out, col_out):
    row_out[...] = row[...].astype(bf16)
    col_out[...] = col[...]


def finish(row, col):
    vmem = pl.BlockSpec(memory_space=pltpu.VMEM)
    return pl.pallas_call(
        finish_kernel,
        out_shape=(jax.ShapeDtypeStruct(row.shape, bf16), jax.ShapeDtypeStruct(col.shape, f32)),
        in_specs=[vmem] * 2, out_specs=(vmem, vmem),
        compiler_params=pltpu.CompilerParams(vmem_limit_bytes=16 << 20))(row, col)


def on_device(n, reps, coords, omega, skeleton):
    leaf, samp = omega.shape
    piece = skeleton.shape[1]
    rank = piece * reps
    cap = -(-max(8, 2 * rank // (n - 1)) // 16) * 16
    if 6 <= n <= 16:
        return finish(*near_call(n, reps, cap, coords, omega, skeleton))
    vmem = pl.BlockSpec(memory_space=pltpu.VMEM)
    sem = pltpu.SemaphoreType.DMA
    row, col = pl.pallas_call(
        functools.partial(kernel, n, reps, cap),
        out_shape=(jax.ShapeDtypeStruct((leaf, samp), f32), jax.ShapeDtypeStruct((leaf, samp), f32)),
        in_specs=[pl.BlockSpec(memory_space=pl.ANY)] * 3,
        out_specs=(vmem, vmem),
        scratch_shapes=[
            pltpu.VMEM(coords.shape, f32),
            pltpu.VMEM(omega.shape, bf16),
            pltpu.VMEM(skeleton.shape, jnp.int32),
            sem((3,)),
            pltpu.VMEM((reps, n, piece), jnp.int32),
            pltpu.VMEM((n, 3, leaf), f32),
            pltpu.VMEM((2, leaf, samp), bf16),
            pltpu.VMEM((2, n, rank), f32),
            pltpu.VMEM((1, rank), f32),
            pltpu.VMEM((n, rank), f32),
            pltpu.VMEM((n, cap, samp), bf16),
            pltpu.VMEM((n, cap, samp), bf16),
            pltpu.VMEM((n, cap, samp), bf16),
            pltpu.VMEM((n, cap, samp), bf16),
            pltpu.VMEM((n, cap, leaf), bf16),
            pltpu.VMEM((n, cap, leaf), bf16),
            pltpu.VMEM((leaf, samp), f32),
            sem((n * reps,)), sem((n * reps,)),
            sem((n,)), sem((n,)), sem((2,)), sem((2,)),
            sem((n,)), sem((n,)), sem((n,)), sem((n,)),
        ],
        compiler_params=pltpu.CompilerParams(collective_id=0, has_side_effects=True),
    )(coords, omega, skeleton)
    return finish(row, col)


def solution(mesh):
    in_specs = (P(None, "node"), P("node", "rep"), P("node", "rep"))
    out_specs = (P("node", "rep"), P("node", "rep"))
    body = functools.partial(on_device, mesh.shape["node"], mesh.shape["rep"])
    return jax.shard_map(body, mesh=mesh, in_specs=in_specs, out_specs=out_specs, check_vma=False)
```

```python
import functools

import jax
import jax.numpy as jnp
from jax import lax
from jax.experimental import pallas as pl
from jax.experimental.pallas import tpu as pltpu
from jax.sharding import PartitionSpec as P

kernel_scale = 0.0078125
softening = 0.02
f32, bf16 = jnp.float32, jnp.bfloat16
MESH = pl.DeviceIdType.MESH


def each(start, stop, body):
    if stop - start <= 8:
        for i in range(start, stop):
            body(i)
    else:
        lax.fori_loop(start, stop, lambda i, c: (body(i), c)[1], 0)


def far_first(n, body):
    half = n // 2
    if n <= 16:
        for d in sorted(range(1, n), key=lambda d: (abs(d - half), d)):
            body(d)
    else:
        each(0, n - 1, lambda d: body(1 + lax.rem(d + half - 1, n - 1)))


def tile(col, row, scale=kernel_scale):
    squared = (col[:, 0:1] - row[0:1, :]) ** 2
    squared = squared + (col[:, 1:2] - row[1:2, :]) ** 2
    squared = squared + (col[:, 2:3] - row[2:3, :]) ** 2
    return (scale * lax.rsqrt(squared + softening * softening)).astype(bf16)


def dot(a, b):
    return jnp.dot(a, b, preferred_element_type=f32)


def kernel(n, reps, cap, coords_in, omega_in, skel_in, row_out, col_out,
           coords, omega, skel, loaded, lists, points, side, keyed, local_req, local_own, rows_out, rows_in, prod_out, prod_in,
           pick_own, far_tile, total,
           list_send, list_recv, point_send, point_recv, side_send, side_recv,
           rows_send, rows_recv, prod_send, prod_recv):
    leaf = coords.shape[1]
    piece = skel.shape[1]
    rank = piece * reps
    me, my_rep = lax.axis_index("node"), lax.axis_index("rep")
    flat = me * reps + my_rep
    count = n * reps

    def at(node, rep):
        return {"node": node, "rep": rep}

    def other(d):
        t = lax.rem(flat + d, count)
        return lax.div(t, reps), lax.rem(t, reps)

    barrier = pltpu.get_barrier_semaphore()

    def greet(d):
        node, rep = other(d)
        pl.semaphore_signal(barrier, inc=1, device_id=at(node, rep), device_id_type=MESH)

    each(1, count, greet)

    loads = [pltpu.make_async_copy(a, b, loaded.at[i]) for i, (a, b) in
             enumerate(((coords_in, coords), (omega_in, omega), (skel_in, skel)))]
    for load in loads:
        load.start()
    for load in loads:
        load.wait()
    own_points = coords[...]
    own_cols = jnp.transpose(jnp.concatenate([own_points, jnp.zeros((5, leaf), f32)], axis=0))
    total[...] = dot(tile(own_cols, own_points), omega[...])
    points[me] = own_points
    lists[my_rep, pl.ds(me, 1)] = skel[...]
    rows_in[me] = jnp.zeros((cap, omega.shape[1]), bf16)
    prod_in[me] = jnp.zeros((cap, omega.shape[1]), bf16)

    pl.semaphore_wait(barrier, count - 1)

    def list_copy(d, node, rep, index):
        return pltpu.make_async_remote_copy(
            src_ref=skel, dst_ref=lists.at[my_rep, pl.ds(me, 1)],
            send_sem=list_send.at[d], recv_sem=list_recv.at[index],
            device_id=at(node, rep), device_id_type=MESH)

    def list_arrival(d):
        node, rep = other(d)
        return pltpu.make_async_remote_copy(
            src_ref=skel, dst_ref=lists.at[rep, pl.ds(node, 1)],
            send_sem=list_send.at[d], recv_sem=list_recv.at[node * reps + rep],
            device_id=at(node, rep), device_id_type=MESH)

    def start_list(d):
        node, rep = other(d)
        list_copy(d, node, rep, flat).start()

    each(1, count, start_list)

    def exchange(d, back, src, dst, send, recv):
        peer = lax.rem(me + d, n)
        place = peer if back else me
        return pltpu.make_async_remote_copy(
            src_ref=src(peer), dst_ref=dst.at[place], send_sem=send.at[peer],
            recv_sem=recv.at[place], device_id=at(peer, my_rep), device_id_type=MESH)

    point_x = lambda d, back=False: exchange(d, back, lambda peer: coords, points, point_send, point_recv)
    rows_x = lambda d, back=False: exchange(d, back, lambda peer: rows_out.at[peer], rows_in, rows_send, rows_recv)
    prod_x = lambda d, back=False: exchange(d, back, lambda peer: prod_out.at[peer], prod_in, prod_send, prod_recv)

    each(1, n, lambda d: point_x(d).start())

    def side_copy(slot):
        peer = me + (1 if slot == 0 else -1)
        return pltpu.make_async_remote_copy(
            src_ref=omega, dst_ref=side.at[slot], send_sem=side_send.at[slot],
            recv_sem=side_recv.at[slot], device_id=at(peer, my_rep), device_id_type=MESH)

    has_above, has_below = me < n - 1, me > 0

    @pl.when(has_above)
    def _():
        side_copy(0).start()

    @pl.when(has_below)
    def _():
        side_copy(1).start()

    each(1, count, lambda d: list_arrival(d).wait_recv())

    listed = jnp.concatenate([lists[r] for r in range(reps)], axis=1)
    mine = jnp.concatenate([lists[r, pl.ds(me, 1)] for r in range(reps)], axis=1)
    local_own[...] = lax.rem(listed, leaf).astype(f32)
    local_req[...] = lax.rem(mine, leaf).astype(f32)
    hit_req = lax.div(mine, leaf) == lax.broadcasted_iota(jnp.int32, (n, rank), 0)
    hit_own = lax.div(listed, leaf) == me
    before = (lax.broadcasted_iota(jnp.int32, (rank, rank), 0)
              < lax.broadcasted_iota(jnp.int32, (rank, rank), 1)).astype(f32).astype(bf16)
    keyed[0] = jnp.where(hit_req, dot(hit_req.astype(f32).astype(bf16), before), -1.0)
    keyed[1] = jnp.where(hit_own, dot(hit_own.astype(f32).astype(bf16), before), -1.0)

    slot_ids = lax.broadcasted_iota(jnp.int32, (cap, rank), 0).astype(f32)
    leaf_ids = lax.broadcasted_iota(jnp.int32, (cap, leaf), 1).astype(f32)

    def picker(keys, local):
        found = jnp.sum(jnp.where(keys == slot_ids, local + 1.0, 0.0), axis=1, keepdims=True)
        return jnp.where(found - 1.0 == leaf_ids, 1.0, 0.0).astype(bf16)

    def send_rows(d):
        peer = lax.rem(me + d, n)
        pick = picker(keyed[1, pl.ds(peer, 1)], local_own[pl.ds(peer, 1)])
        pick_own[peer] = pick
        rows_out[peer] = dot(pick, omega[...]).astype(bf16)
        rows_x(d).start()

    def send_products(d):
        peer = lax.rem(me + d, n)
        point_x(d, True).wait_recv()
        pick = picker(keyed[0, pl.ds(peer, 1)], local_req[...])
        whole = points[peer]
        high = whole.astype(bf16).astype(f32)
        middle = (whole - high).astype(bf16).astype(f32)
        low = whole - high - middle
        parts = jnp.concatenate([high, middle, low], axis=0).astype(bf16)
        got = lax.dot_general(pick, parts, (((1,), (1,)), ((), ())), preferred_element_type=f32)
        slots = got[:, 0:3] + got[:, 3:6] + got[:, 6:9]
        skel_tile = tile(slots, own_points)
        far_tile[peer] = skel_tile
        prod_out[peer] = dot(skel_tile, omega[...]).astype(bf16)
        prod_x(d).start()

    far_first(n, send_rows)
    pick_own[me] = jnp.zeros((cap, leaf), bf16)
    far_tile[me] = jnp.zeros((cap, leaf), bf16)
    far_first(n, send_products)

    @pl.when(has_below)
    def _():
        side_copy(0).wait_recv()
        total[...] += dot(tile(own_cols, points[jnp.maximum(me - 1, 0)]), side[0])

    @pl.when(has_above)
    def _():
        side_copy(1).wait_recv()
        total[...] += dot(tile(own_cols, points[jnp.minimum(me + 1, n - 1)]), side[1])

    far = far_tile[...].reshape(n * cap, leaf).T
    back = pick_own[...].reshape(n * cap, leaf).T

    each(1, n, lambda d: rows_x(d, True).wait_recv())
    row_out[...] = (total[...] + dot(far, rows_in[...].reshape(n * cap, -1)))
    each(1, n, lambda d: prod_x(d, True).wait_recv())
    col_out[...] = dot(back, prod_in[...].reshape(n * cap, -1))

    each(1, count, lambda d: list_arrival(d).wait_send())
    each(1, n, lambda d: point_x(d).wait_send())
    each(1, n, lambda d: rows_x(d).wait_send())
    each(1, n, lambda d: prod_x(d).wait_send())

    @pl.when(has_above)
    def _():
        side_copy(0).wait_send()

    @pl.when(has_below)
    def _():
        side_copy(1).wait_send()


def near_kernel(n, reps, cap, sent, coords_in, omega_in, skel_in, row_out, col_out,
                coords, omega, skel, pieces, code_out, code_in, points, side, rows_out, rows_in, prod_out,
                prod_in, pick_own, pick_req, far_tile, near_tile, edge_tile, edge_prod, total,
                loaded, piece_send, piece_recv, point_send, code_send, point_recv, code_recv,
                side_send, side_recv, rows_send, rows_recv, prod_send, prod_recv, ready, mates):
    leaf, samp = omega.shape
    rank = skel.shape[1] * reps
    me, my_rep = lax.axis_index("node"), lax.axis_index("rep")
    first, last = (n - me) // n, (me + 1) // n
    edge = first + last
    beside = (1, -1)
    parts, slots = 2, n - 2
    late = range(3, n)

    def peer_of(k):
        before_me = (me + n - k - 2) // n
        return before_me * k + (1 - before_me) * (3 + k - first)

    peers = [peer_of(k) for k in range(n - 3)]
    peers.append(edge * peer_of(n - 3) + (1 - edge) * me)

    def if_edge(body):
        @pl.when(edge == 1)
        def _():
            body()

    def if_there(offset, body):
        @pl.when(me + offset < n if offset > 0 else me + offset >= 0)
        def _():
            body()

    def signal(sem, node, rep):
        pl.semaphore_signal(sem, inc=1, device_id={"node": node, "rep": rep}, device_id_type=MESH)

    def send(src, dst, send_sem, recv_sem, node, rep):
        return pltpu.make_async_remote_copy(
            src_ref=src, dst_ref=dst, send_sem=send_sem, recv_sem=recv_sem,
            device_id={"node": node, "rep": rep}, device_id_type=MESH)

    def wait(like, sem):
        pltpu.make_async_copy(like, like, sem).wait()

    def point_x(peer):
        return send(coords, points.at[me], point_send, point_recv.at[me], peer, my_rep)

    def code_x(peer):
        return send(code_out.at[peer], code_in.at[me], code_send, code_recv.at[me], peer, my_rep)

    def hinted(peer):
        wait(coords, point_recv.at[peer])
        wait(code_out.at[0], code_recv.at[peer])

    def rows_x(peer):
        return send(rows_out.at[peer, pl.ds(0, sent)], rows_in.at[me, pl.ds(0, sent)], rows_send, rows_recv, peer, my_rep)

    def prod_x(peer):
        return send(prod_out.at[peer, pl.ds(0, sent)], prod_in.at[me, pl.ds(0, sent)], prod_send, prod_recv, peer, my_rep)

    def push(slot, part):
        rows = pl.ds(part * (leaf // parts), leaf // parts)
        send(omega.at[rows], side.at[1 - slot, rows], side_send.at[slot], side_recv.at[1 - slot], me + beside[slot], my_rep).start()

    def piece_x(rep):
        return send(skel, pieces.at[my_rep], piece_send, piece_recv, me, rep)

    loads = [pltpu.make_async_copy(a, b, loaded.at[i]) for i, (a, b) in
             enumerate(((skel_in, skel), (coords_in, coords), (omega_in, omega)))]
    for load in loads:
        load.start()

    barrier = pltpu.get_barrier_semaphore()
    for o in range(1, n):
        if_there(o, lambda o=o: signal(barrier, me + o, my_rep))
    for r in range(1, reps):
        @pl.when(my_rep < r)
        def _():
            signal(barrier, me, r)

    with jax.named_scope("enter"):
        @pl.when(me + my_rep > 0)
        def _():
            pl.semaphore_wait(barrier, me + my_rep)

    for r in range(reps - 1):
        @pl.when(my_rep > r)
        def _():
            signal(mates, me, r)
    for o in range(1, n):
        if_there(-o, lambda o=o: signal(ready.at[me], me - o, my_rep))

    with jax.named_scope("load"):
        loads[0].wait()
    for r in range(reps - 1):
        @pl.when(my_rep > r)
        def _():
            piece_x(r).start()
    loads[1].wait()
    for o in range(1, n):
        if_there(-o, lambda o=o: point_x(me - o).start())
    loads[2].wait()
    if_there(-1, lambda: push(1, 0))

    own_points = coords[...]
    own_cols = jnp.transpose(jnp.concatenate([own_points, jnp.zeros((5, leaf), f32)], axis=0))
    pieces[my_rep] = skel[...]
    rows_in[...] = jnp.zeros((n, cap, samp), bf16)
    prod_in[...] = jnp.zeros((n, cap, samp), bf16)
    edge_prod[...] = jnp.zeros((2, cap, samp), bf16)
    far_tile[slots - 1] = jnp.zeros((cap, leaf), bf16)
    for k in range(slots - 1, n):
        pick_own[k] = jnp.zeros((cap, leaf), bf16)

    with jax.named_scope("own"):
        total[...] = dot(tile(own_cols, own_points), omega[...])

    with jax.named_scope("mates"):
        @pl.when(my_rep < reps - 1)
        def _():
            pl.semaphore_wait(mates, reps - 1 - my_rep)
    for r in range(1, reps):
        @pl.when(my_rep < r)
        def _():
            piece_x(r).start()

    def meet(o):
        with jax.named_scope(f"ready{o}"):
            pl.semaphore_wait(ready.at[me + o], 1)
        point_x(me + o).start()
        if o == 1:
            push(0, 0)

    for o in (1, 2):
        if_there(o, lambda o=o: meet(o))

    with jax.named_scope("pieces"):
        wait(pieces.at[pl.ds(0, reps - 1)], piece_recv)
    mine = jnp.concatenate([pieces[r] for r in range(reps)], axis=1)
    local = lax.rem(mine, leaf).astype(f32)
    before = (lax.broadcasted_iota(jnp.int32, (rank, rank), 0)
              < lax.broadcasted_iota(jnp.int32, (rank, rank), 1)).astype(f32).astype(bf16)
    hit = lax.div(mine, leaf) == lax.broadcasted_iota(jnp.int32, (n, rank), 0)
    keys = jnp.where(hit, dot(hit.astype(f32).astype(bf16), before), -1.0)
    codes = jnp.where(hit, (keys + 1.0) * leaf + local, 0.0).astype(jnp.int32)
    for i in range(n):
        code_out[i] = codes[i:i + 1]
    for o in (*range(-n + 1, 0), 1, 2):
        if_there(o, lambda o=o: code_x(me + o).start())
    for o in range(3, n):
        def follow(o=o):
            meet(o)
            code_x(me + o).start()
        if_there(o, follow)
    for slot in (0, 1):
        if_there(beside[slot], lambda slot=slot: push(slot, 1))

    slot_ids = lax.broadcasted_iota(jnp.int32, (cap, rank), 0).astype(f32)
    leaf_ids = lax.broadcasted_iota(jnp.int32, (cap, leaf), 1).astype(f32)

    def picker(key, index):
        found = jnp.sum(jnp.where(key == slot_ids, index + 1.0, 0.0), axis=1, keepdims=True)
        return jnp.where(found - 1.0 == leaf_ids, 1.0, 0.0).astype(bf16)

    def places(pick, whole):
        high = whole.astype(bf16).astype(f32)
        middle = (whole - high).astype(bf16).astype(f32)
        low = whole - high - middle
        parts = jnp.concatenate([high, middle, low], axis=0).astype(bf16)
        got = lax.dot_general(pick, parts, (((1,), (1,)), ((), ())), preferred_element_type=f32)
        return got[:, 0:3] + got[:, 3:6] + got[:, 6:9]

    def asked(peer):
        code = code_in[peer]
        return picker((lax.div(code, leaf) - 1).astype(f32), lax.rem(code, leaf).astype(f32))

    with jax.named_scope("requests"):
        for i in range(n):
            pick_req[i] = picker(keys[i:i + 1], local)

    def serve(group):
        with jax.named_scope("wait" + "".join(map(str, group))):
            for k in group:
                hinted(peers[k])
        with jax.named_scope("serve" + "".join(map(str, group))):
            picks = [asked(peers[k]) for k in group]
            tiles = [tile(places(pick_req[peers[k]], points[peers[k]]), own_points) for k in group]
            for k, pick in zip(group, picks):
                pick_own[k] = pick
                rows_out[peers[k]] = dot(pick, omega[...]).astype(bf16)
            for k, skel_tile in zip(group, tiles):
                far_tile[k] = skel_tile
                prod_out[peers[k]] = dot(skel_tile, omega[...]).astype(bf16)
        for k in group:
            rows_x(peers[k]).start()
            prod_x(peers[k]).start()

    for group in ([0], *([k, k + 1] for k in range(1, n - 4, 2)), *([[n - 4]] if n % 2 else [])):
        serve(group)
    if_edge(lambda: serve([n - 3]))

    def prepare(slot):
        peer = me + beside[slot]
        with jax.named_scope(f"besidewait{slot}"):
            hinted(peer)
        with jax.named_scope(f"beside{slot}"):
            there = points[peer]
            counted = jnp.sum(pick_req[peer].astype(f32), axis=0, keepdims=True) + 1.0
            near_tile[slot] = tile(own_cols, there, kernel_scale * counted)
            pick = asked(peer)
            pick_own[slots + slot] = pick
            edge_tile[slot] = tile(places(pick, own_points), there)

    def collect(slot):
        with jax.named_scope(f"side{slot}"):
            wait(side.at[slot], side_recv.at[slot])
        with jax.named_scope(f"near{slot}"):
            edge_prod[slot] = dot(edge_tile[slot], side[slot]).astype(bf16)
            total[...] += dot(near_tile[slot], side[slot])

    for slot in (0, 1):
        if_there(beside[slot], lambda slot=slot: prepare(slot))

    with jax.named_scope("turn"):
        far = far_tile[...].reshape(slots * cap, leaf).T
        back = pick_own[...].reshape(n * cap, leaf).T

    with jax.named_scope("sent"):
        wait(pieces.at[pl.ds(0, reps - 1)], piece_send)
        wait(points.at[pl.ds(0, n - 1)], point_send)
        wait(code_out.at[pl.ds(0, n - 1)], code_send)

    for slot in (0, 1):
        if_there(beside[slot], lambda slot=slot: collect(slot))

    def gather(like, sem):
        def some(count):
            wait(like.at[pl.ds(0, count), pl.ds(0, sent)], sem)

        @pl.when(edge == 1)
        def _():
            some(n - 2)

        @pl.when(edge == 0)
        def _():
            some(n - 3)

    with jax.named_scope("rows"):
        gather(rows_in, rows_recv)
    with jax.named_scope("rowsum"):
        row_out[...] = total[...] + dot(far, jnp.concatenate([rows_in[p] for p in peers], axis=0))
    with jax.named_scope("prods"):
        gather(prod_in, prod_recv)
    with jax.named_scope("colsum"):
        col_out[...] = dot(back, jnp.concatenate([prod_in[p] for p in peers] + [edge_prod[0], edge_prod[1]], axis=0))

    with jax.named_scope("sent2"):
        for slot in (0, 1):
            if_there(beside[slot], lambda slot=slot: wait(omega, side_send.at[slot]))
        gather(rows_out, rows_send)
        gather(prod_out, prod_send)


def near_call(n, reps, cap, coords, omega, skeleton):
    leaf, samp = omega.shape
    piece = skeleton.shape[1]
    need = max(8, 2 * piece * reps // (n - 1))
    sent = need + need % 2
    vmem = pl.BlockSpec(memory_space=pltpu.VMEM)
    sem = pltpu.SemaphoreType.DMA
    return pl.pallas_call(
        functools.partial(near_kernel, n, reps, cap, sent),
        out_shape=(pltpu.VMEM((leaf, samp), f32), pltpu.VMEM((leaf, samp), f32)),
        in_specs=[pl.BlockSpec(memory_space=pltpu.HBM)] * 3,
        out_specs=(vmem, vmem),
        scratch_shapes=[
            pltpu.VMEM(coords.shape, f32),
            pltpu.VMEM(omega.shape, bf16),
            pltpu.VMEM(skeleton.shape, jnp.int32),
            pltpu.VMEM((reps, 1, piece), jnp.int32),
            pltpu.VMEM((n, 1, piece * reps), jnp.int32),
            pltpu.VMEM((n, 1, piece * reps), jnp.int32),
            pltpu.VMEM((n, 3, leaf), f32),
            pltpu.VMEM((2, leaf, samp), bf16),
            pltpu.VMEM((n, cap, samp), bf16),
            pltpu.VMEM((n, cap, samp), bf16),
            pltpu.VMEM((n, cap, samp), bf16),
            pltpu.VMEM((n, cap, samp), bf16),
            pltpu.VMEM((n, cap, leaf), bf16),
            pltpu.VMEM((n, cap, leaf), bf16),
            pltpu.VMEM((n - 2, cap, leaf), bf16),
            pltpu.VMEM((2, leaf, leaf), bf16),
            pltpu.VMEM((2, cap, leaf), bf16),
            pltpu.VMEM((2, cap, samp), bf16),
            pltpu.VMEM((leaf, samp), f32),
            sem((3,)), sem, sem, sem, sem, sem((n,)), sem((n,)), sem((2,)), sem((2,)),
            sem, sem, sem, sem,
            pltpu.SemaphoreType.REGULAR((n,)), pltpu.SemaphoreType.REGULAR,
        ],
        compiler_params=pltpu.CompilerParams(collective_id=0, has_side_effects=True),
    )(coords, omega, skeleton)


def finish_kernel(row, col, row_out, col_out):
    row_out[...] = row[...].astype(bf16)
    col_out[...] = col[...]


def finish(row, col):
    vmem = pl.BlockSpec(memory_space=pltpu.VMEM)
    return pl.pallas_call(
        finish_kernel,
        out_shape=(jax.ShapeDtypeStruct(row.shape, bf16), jax.ShapeDtypeStruct(col.shape, f32)),
        in_specs=[vmem] * 2, out_specs=(vmem, vmem),
        compiler_params=pltpu.CompilerParams(vmem_limit_bytes=16 << 20))(row, col)


def on_device(n, reps, coords, omega, skeleton):
    leaf, samp = omega.shape
    piece = skeleton.shape[1]
    rank = piece * reps
    cap = -(-max(8, 2 * rank // (n - 1)) // 16) * 16
    if 6 <= n <= 16:
        return finish(*near_call(n, reps, cap, coords, omega, skeleton))
    vmem = pl.BlockSpec(memory_space=pltpu.VMEM)
    sem = pltpu.SemaphoreType.DMA
    row, col = pl.pallas_call(
        functools.partial(kernel, n, reps, cap),
        out_shape=(jax.ShapeDtypeStruct((leaf, samp), f32), jax.ShapeDtypeStruct((leaf, samp), f32)),
        in_specs=[pl.BlockSpec(memory_space=pl.ANY)] * 3,
        out_specs=(vmem, vmem),
        scratch_shapes=[
            pltpu.VMEM(coords.shape, f32),
            pltpu.VMEM(omega.shape, bf16),
            pltpu.VMEM(skeleton.shape, jnp.int32),
            sem((3,)),
            pltpu.VMEM((reps, n, piece), jnp.int32),
            pltpu.VMEM((n, 3, leaf), f32),
            pltpu.VMEM((2, leaf, samp), bf16),
            pltpu.VMEM((2, n, rank), f32),
            pltpu.VMEM((1, rank), f32),
            pltpu.VMEM((n, rank), f32),
            pltpu.VMEM((n, cap, samp), bf16),
            pltpu.VMEM((n, cap, samp), bf16),
            pltpu.VMEM((n, cap, samp), bf16),
            pltpu.VMEM((n, cap, samp), bf16),
            pltpu.VMEM((n, cap, leaf), bf16),
            pltpu.VMEM((n, cap, leaf), bf16),
            pltpu.VMEM((leaf, samp), f32),
            sem((n * reps,)), sem((n * reps,)),
            sem((n,)), sem((n,)), sem((2,)), sem((2,)),
            sem((n,)), sem((n,)), sem((n,)), sem((n,)),
        ],
        compiler_params=pltpu.CompilerParams(collective_id=0, has_side_effects=True),
    )(coords, omega, skeleton)
    return finish(row, col)


def solution(mesh):
    in_specs = (P(None, "node"), P("node", "rep"), P("node", "rep"))
    out_specs = (P("node", "rep"), P("node", "rep"))
    body = functools.partial(on_device, mesh.shape["node"], mesh.shape["rep"])
    return jax.shard_map(body, mesh=mesh, in_specs=in_specs, out_specs=out_specs, check_vma=False)
```
